32 devices in a mesh: dp: 4 (over y, x), fsdp: 8 (over z, core).
Axes of the slice: x: 2, y: 2, z: 4, core: 2. Of those that a mesh axis runs over, the one named last changes fastest.
Arguments:
- tokens: bfloat16 [512, 3072], P('dp'), may hold values from -6 to 6
- cotangent: bfloat16 [512, 3072], P('dp'), may hold values from -6 to 6
- routes: int32 [512, 2], P('dp'), may hold values from 0 to 3, all different within a row; in each aligned block of 128 rows (0 to 127, 128 to 255, ...) at most 64 rows name the same one
- router_weight: float32 [512, 2], P('dp'), may hold values from 0.25 to 1
- w_gate: bfloat16 [4, 3072, 8192], P('dp', None, 'fsdp'), may hold values from -0.109375 to 0.109375
- w_up: bfloat16 [4, 3072, 8192], P('dp', None, 'fsdp'), may hold values from -0.109375 to 0.109375
- w_down: bfloat16 [4, 8192, 3072], P('dp', 'fsdp'), may hold values from -0.0625 to 0.0625
Outputs:
- output: bfloat16 [512, 3072], P('dp')
- input_grad: bfloat16 [512, 3072], P('dp')
- grad_gate: bfloat16 [4, 3072, 8192], P('dp', None, 'fsdp')
- grad_up: bfloat16 [4, 3072, 8192], P('dp', None, 'fsdp')
- grad_down: bfloat16 [4, 8192, 3072], P('dp', 'fsdp')
The draws below stay inside these ranges and needn't reach their ends.
Inputs may be any that keep to these rules, and one draw needn't show every extreme that they name: `routes`: the two experts of a token differ. In the 128 rows of one batch no expert is named by more than 64 rows, a bound that some block reaches in some batches.
All inputs are finite; a program needn't handle non-finite values.
Results may differ from the reference program's by a relative error of at most 0.025.
Values may be sent and summed in bfloat16 or wider, within the bound.
A program may use at most 128 MiB of HBM per device.

```python
import math
import jax
import jax.numpy as jnp
import numpy as np
from jax import lax

D = 3072
F = 8192
TOK_DEV = 128
EXPERTS = 4
CAP = 64
TOKENS = 512
N_DP = 4
N_FSDP = 8


def levels(rng, shape, shards, low, top_value):
    level = 1.0
    for dim, parts in shards:
        heights = jax.random.uniform(jax.random.fold_in(jax.random.fold_in(rng, 6), dim), (parts,), jnp.float32, low / len(shards), top_value / len(shards))
        level = level * jnp.repeat(jnp.exp(heights), shape[dim] // parts).reshape((-1,) + (1,) * (len(shape) - 1 - dim))
    return level


def assign_block(stream_key, own, number, rows, count, top, limit, lean):
    sequence = jax.random.permutation(stream_key, count)
    crowded, common = portions_of(count, rows * top, limit, lean, True), portions_of(count, rows * top, limit, lean, False)
    places = jnp.arange(count)

    def named(lengths, offset_by):
        used = int((lengths > 0).sum())
        fixed = max(1, used // 4)
        passed = fixed + (places - fixed + offset_by * (used - fixed)) % max(1, count - fixed)
        return jnp.zeros((count,), jnp.int32).at[sequence[jnp.where(places < fixed, places, passed)]].set(jnp.asarray(lengths, jnp.int32))

    lengths = jnp.where(number % 4 == 0, named(crowded, number // 4), named(common, number - number // 4 - 1))
    mixed = jax.random.permutation(jax.random.fold_in(own, 3), count)
    source_of, sink = mixed[0:count // 2 * 2:2], mixed[1:count // 2 * 2:2]
    room = jnp.minimum(lengths[source_of] - 1, limit - lengths[sink]) // 2
    room = jnp.where((source_of == sequence[0]) | (sink == sequence[0]) | (lengths[sink] == 0), 0, jnp.maximum(room, 0))
    passed = jax.random.randint(jax.random.fold_in(own, 4), (count // 2,), 0, 1 << 20) % (room + 1)
    lengths = lengths.at[source_of].add(-passed).at[sink].add(passed)
    labels = jnp.searchsorted(jnp.cumsum(lengths), jnp.arange(rows * top), side="right").astype(jnp.int32)
    grid = labels.reshape(top, rows).T
    grid = grid[jax.random.permutation(jax.random.fold_in(own, 1), rows)]
    offset_by = jax.random.randint(jax.random.fold_in(own, 2), (rows, 1), 0, top)
    return jnp.take_along_axis(grid, (jnp.arange(top)[None, :] + offset_by) % top, axis=1)


def portions_of(number_of, total, bound, skew, full):
    portions = [(1 << 20) // math.isqrt(grade ** skew) + 1 for grade in range(1, number_of + 1)]
    largest = bound if full else min(bound, max(-(-total // number_of), total * portions[0] // sum(portions)))
    least = 1 if total - largest >= number_of - 1 else 0
    given, surplus = [largest] + [least] * (number_of - 1), total - largest - least * (number_of - 1)
    while surplus > 0:
        candidates = [i for i in range(1, number_of) if given[i] < largest] or [i for i in range(1, number_of) if given[i] < bound]
        whole, budget = sum([portions[i] for i in candidates]), surplus
        for i in candidates:
            extra = min(bound - given[i], max(1, budget * portions[i] // whole), surplus)
            given[i] = given[i] + extra
            surplus = surplus - extra
    return np.array(given)


def bell_draw(key, extent, width, bound, split=(), kind=jnp.bfloat16):
    gain = levels(key, extent, split, -0.22, 0.18) if split else 1.0
    entries = jax.random.normal(key, extent, jnp.float32) * width * gain
    return jnp.minimum(jnp.maximum(entries, -bound), bound).astype(kind)


def setup_inputs(seed: int = 0) -> dict:
    seeds = jax.random.split(jax.random.key(seed), 8)
    tokens = bell_draw(seeds[0], (TOKENS, D), 1.0, 6.0, ((0, 4),))
    cotangent = bell_draw(seeds[1], (TOKENS, D), 1.0, 6.0, ((0, 4),))
    routes_keys = jax.random.split(jax.random.fold_in(seeds[2], 1), TOKENS // TOK_DEV)
    routes_turns = jax.random.permutation(jax.random.fold_in(seeds[2], 3), TOKENS // TOK_DEV)
    routes = jax.vmap(lambda own, number: assign_block(jax.random.fold_in(seeds[2], 2), own, number, TOK_DEV, N_DP, 2, CAP, 1))(routes_keys, routes_turns).reshape((TOKENS, 2))
    router_weight = jnp.clip(0.25 + 0.75 * jax.random.uniform(seeds[3], (TOKENS, 2), jnp.float32) ** levels(seeds[3], (TOKENS, 2), ((0, 4),), -0.2, 0.2), 0.25, 1.0)
    w_gate = bell_draw(seeds[4], (EXPERTS, D, F), D ** -0.5, 0.109375, ((0, 4), (2, 8)))
    w_up = bell_draw(seeds[5], (EXPERTS, D, F), D ** -0.5, 0.109375, ((0, 4), (2, 8)))
    w_down = bell_draw(seeds[6], (EXPERTS, F, D), F ** -0.5, 0.0625, ((0, 4), (1, 8)))
    return dict(tokens=tokens, cotangent=cotangent, routes=routes, router_weight=router_weight, w_gate=w_gate, w_up=w_up, w_down=w_down)


def slot_tables(routes, router_weight):
    expert_ids = jnp.arange(N_DP, dtype=jnp.int32)
    hit_table = (routes[..., None] == expert_ids).astype(jnp.int32)
    per_token = jnp.sum(hit_table, axis=2)
    before = jnp.cumsum(per_token, axis=1) - per_token
    slot_of = jnp.sum(hit_table * before[:, :, None, :], axis=3)
    slot_ids = jnp.arange(CAP, dtype=jnp.int32)
    placed = hit_table[..., None] * (slot_of[..., None, None] == slot_ids).astype(jnp.int32)
    picked = jnp.sum(placed, axis=2).astype(jnp.float32)
    weighted = jnp.sum(placed.astype(jnp.float32) * router_weight[..., None, None], axis=2)
    return picked, weighted


def expert_pass(operands):
    slot_x, slot_dy, gate_w, up_w, down_w = operands
    gate_pre = jnp.dot(slot_x, gate_w, preferred_element_type=jnp.float32)
    up_pre = jnp.dot(slot_x, up_w, preferred_element_type=jnp.float32)
    sigma = jax.nn.sigmoid(gate_pre)
    active = gate_pre * sigma
    hidden = (active * up_pre).astype(jnp.bfloat16)
    hidden_dy = jnp.dot(slot_dy, down_w.T, preferred_element_type=jnp.float32)
    gate_dy = (hidden_dy * up_pre * sigma * (1.0 + gate_pre * (1.0 - sigma))).astype(jnp.bfloat16)
    up_dy = (hidden_dy * active).astype(jnp.bfloat16)
    grad_down = jnp.dot(hidden.T, slot_dy, preferred_element_type=jnp.float32).astype(jnp.bfloat16)
    grad_gate = jnp.dot(slot_x.T, gate_dy, preferred_element_type=jnp.float32).astype(jnp.bfloat16)
    grad_up = jnp.dot(slot_x.T, up_dy, preferred_element_type=jnp.float32).astype(jnp.bfloat16)
    block_width = F // N_FSDP

    def one_block(carry, index):
        start = (index * block_width).astype(jnp.int32)
        hidden_part = lax.dynamic_slice_in_dim(hidden, start, block_width, 1)
        gate_part = lax.dynamic_slice_in_dim(gate_dy, start, block_width, 1)
        up_part = lax.dynamic_slice_in_dim(up_dy, start, block_width, 1)
        down_rows = lax.dynamic_slice_in_dim(down_w, start, block_width, 0)
        gate_cols = lax.dynamic_slice_in_dim(gate_w, start, block_width, 1)
        up_cols = lax.dynamic_slice_in_dim(up_w, start, block_width, 1)
        out_term = jnp.dot(hidden_part, down_rows, preferred_element_type=jnp.float32).astype(jnp.bfloat16)
        out_term = lax.optimization_barrier(out_term)
        back_term = (jnp.dot(gate_part, gate_cols.T, preferred_element_type=jnp.float32)
                     + jnp.dot(up_part, up_cols.T, preferred_element_type=jnp.float32)).astype(jnp.bfloat16)
        back_term = lax.optimization_barrier(back_term)
        return (carry[0] + out_term.astype(jnp.float32), carry[1] + back_term.astype(jnp.float32)), None

    zeros = jnp.zeros((slot_x.shape[0], D), jnp.float32)
    totals, unused = lax.scan(one_block, (zeros, zeros), jnp.arange(N_FSDP, dtype=jnp.int32))
    return totals[0].astype(jnp.bfloat16), totals[1].astype(jnp.bfloat16), grad_gate, grad_up, grad_down


def reference(tokens, cotangent, routes, router_weight, w_gate, w_up, w_down):
    blocks = TOKENS // TOK_DEV
    highest = lax.Precision.HIGHEST
    inputs = tokens.reshape(blocks, TOK_DEV, D).astype(jnp.float32)
    grads_in = cotangent.reshape(blocks, TOK_DEV, D).astype(jnp.float32)
    picked, weighted = slot_tables(routes.reshape(blocks, TOK_DEV, 2), router_weight.reshape(blocks, TOK_DEV, 2))
    slot_x = jnp.einsum('btec,btd->ebcd', picked, inputs, precision=highest).astype(jnp.bfloat16)
    slot_dy = jnp.einsum('btec,btd->ebcd', weighted, grads_in, precision=highest).astype(jnp.bfloat16)
    slot_x = slot_x.reshape(N_DP, blocks * CAP, D)
    slot_dy = slot_dy.reshape(N_DP, blocks * CAP, D)
    slot_out, slot_dx, grad_gate, grad_up, grad_down = lax.map(expert_pass, (slot_x, slot_dy, w_gate, w_up, w_down))
    slot_out = slot_out.reshape(N_DP, blocks, CAP, D).astype(jnp.float32)
    slot_dx = slot_dx.reshape(N_DP, blocks, CAP, D).astype(jnp.float32)
    output = jnp.einsum('btec,ebcd->btd', weighted, slot_out, precision=highest).astype(jnp.bfloat16)
    input_grad = jnp.einsum('btec,ebcd->btd', picked, slot_dx, precision=highest).astype(jnp.bfloat16)
    return (output.reshape(TOKENS, D), input_grad.reshape(TOKENS, D), grad_gate, grad_up, grad_down)
```

```python
import functools

import jax
import jax.numpy as jnp
from jax import lax
from jax.experimental import pallas as pl
from jax.experimental.pallas import tpu as pltpu
from jax.sharding import PartitionSpec as P

MESH = pl.DeviceIdType.MESH
BF16 = jnp.bfloat16
F32 = jnp.float32
LEAD = (((0,), (0,)), ((), ()))
TRAIL = (((1,), (1,)), ((), ()))


def flip(a, mask):
    bit = 1
    while bit <= mask:
        if mask & bit:
            a = a + bit - 2 * bit * ((a // bit) % 2)
        bit *= 2
    return a


def mm(a, b, dims=(((1,), (0,)), ((), ()))):
    return lax.dot_general(a, b, dims, preferred_element_type=F32)


def routed_kernel(
    n, nz, cap, tile,
    tokens, cotangent, routes_t, rweight_t, rweight, wg_hbm, wu_hbm, wd_hbm,
    output, input_grad, slots_hbm, hidden_hbm,
    wg, wu, wd, slots, snd, gpre, upre, hid,
    core_snd, core_rcv, own, ret_snd, ret, zacc, zsnd, zrcv, fin,
    w_sem, a_send, a_recv, f_send, f_recv, c_send, c_recv, r_send, r_recv,
    z_send, z_recv, g_send, g_recv, h_send, h_recv, o_sem,
):
    d = lax.axis_index("dp")
    f = lax.axis_index("fsdp")
    c = f % 2
    z = f // 2
    sib = (d, flip(f, 1))
    toks, features = tokens.shape
    half = features // 2
    rows = n * cap
    units = hid.shape[2]
    order = sorted(range(1, n), key=lambda m: -bin(m).count("1"))
    bits = [1 << s for s in range(nz.bit_length() - 1)]

    def remote(src, dst, ssem, rsem, dev):
        return pltpu.make_async_remote_copy(
            src_ref=src, dst_ref=dst, send_sem=ssem, recv_sem=rsem,
            device_id=dev, device_id_type=MESH,
        )

    loads = [
        pltpu.make_async_copy(s, t, w_sem.at[k])
        for k, (s, t) in enumerate(((wg_hbm, wg), (wu_hbm, wu), (wd_hbm, wd)))
    ]
    for load in loads:
        load.start()

    barrier = pltpu.get_barrier_semaphore()
    friends = [(flip(d, m), f) for m in order] + [sib] + [(d, flip(f, 2 * b)) for b in bits]
    for dev in friends:
        pl.semaphore_signal(barrier, inc=1, device_id=dev, device_id_type=MESH)

    slot_row = lax.broadcasted_iota(jnp.int32, (rows, toks), 0)
    e_of = slot_row // cap
    s_of = (slot_row % cap).astype(F32)
    r = routes_t[...]
    hit0 = r[0:1, :] == e_of
    hit1 = r[1:2, :] == e_of
    per_token = jnp.where(hit0 | hit1, 1.0, 0.0).astype(BF16)
    earlier = (
        lax.broadcasted_iota(jnp.int32, (toks, toks), 0)
        < lax.broadcasted_iota(jnp.int32, (toks, toks), 1)
    )
    before = mm(per_token, jnp.where(earlier, 1.0, 0.0).astype(BF16))
    here = before == s_of
    first = jnp.where(hit0 & here, 1.0, 0.0)
    second = jnp.where(hit1 & here, 1.0, 0.0)
    rw = rweight_t[...]
    slot_weight = jnp.sum(first * rw[0:1, :] + second * rw[1:2, :], axis=1, keepdims=True)
    first = first.astype(BF16)
    second = second.astype(BF16)
    picked = first + second

    mine = pl.ds(pl.multiple_of(c * half, 128), half)
    snd[0] = mm(picked, tokens[:, mine]).astype(BF16).reshape(n, cap, half)
    pl.semaphore_wait(barrier, len(friends))

    sends = []

    def dispatch(t):
        for m in order:
            e = flip(d, m)
            cp = remote(snd.at[t, e], slots.at[c, t, d], a_send.at[t, m], a_recv.at[t, m], (e, f))
            cp.start()
            sends.append(cp)
        slots[c, t, d] = snd[t, d]

    def share(t):
        for m in [0] + order:
            b = flip(d, m)
            if m:
                remote(
                    snd.at[t, b], slots.at[c, t, b], a_send.at[t, m], a_recv.at[t, m], (b, f)
                ).wait_recv()
            cp = remote(slots.at[c, t, b], slots.at[c, t, b], f_send.at[t, m], f_recv.at[t, m], sib)
            cp.start()
            sends.append(cp)

    def shared(t):
        for m in [0] + order:
            b = flip(d, m)
            remote(
                slots.at[1 - c, t, b], slots.at[1 - c, t, b], f_send.at[t, m], f_recv.at[t, m], sib
            ).wait_recv()

    dispatch(0)
    snd[1] = (mm(picked, cotangent[:, mine]) * slot_weight).astype(BF16).reshape(n, cap, half)
    dispatch(1)
    share(0)
    shared(0)
    loads[0].wait()
    loads[1].wait()

    def up_step(j, carry):
        cols = pl.ds(pl.multiple_of(j * tile, tile), tile)
        x0 = slots[0, 0].reshape(rows, half)
        x1 = slots[1, 0].reshape(rows, half)
        g = mm(x0, wg[pl.ds(0, half), cols]) + mm(x1, wg[pl.ds(half, half), cols])
        u = mm(x0, wu[pl.ds(0, half), cols]) + mm(x1, wu[pl.ds(half, half), cols])
        gpre[:, cols] = g
        upre[:, cols] = u
        hid[0, :, cols] = (g * jax.nn.sigmoid(g) * u).astype(BF16)
        return carry

    lax.fori_loop(0, units // tile, up_step, 0)
    loads[2].wait()

    def project(t, term):
        def theirs(k, carry):
            cols = pl.ds(pl.multiple_of(k * tile, tile), tile)
            v = term(pl.ds(pl.multiple_of((1 - c) * half + k * tile, tile), tile))
            core_snd[t, :, :, cols] = v.astype(BF16).reshape(n, cap, tile)
            return carry

        def ours(k, carry):
            cols = pl.ds(pl.multiple_of(k * tile, tile), tile)
            own[t, :, cols] = term(pl.ds(pl.multiple_of(c * half + k * tile, tile), tile))
            return carry

        lax.fori_loop(0, half // tile, theirs, 0)
        cp = remote(core_snd.at[t], core_rcv.at[t], c_send.at[t], c_recv.at[t], sib)
        cp.start()
        lax.fori_loop(0, half // tile, ours, 0)
        cp.wait_recv()
        sends.append(cp)
        for m in order + [0]:
            b = flip(d, m)
            at = pl.ds(pl.multiple_of(b * cap, 16), cap)
            v = (own[t, at, :] + core_rcv[t, b].astype(F32)).astype(BF16)
            if m:
                ret_snd[t, b] = v
                cp = remote(ret_snd.at[t, b], ret.at[t, d], r_send.at[t, m], r_recv.at[t, m], (b, f))
                cp.start()
                sends.append(cp)
            else:
                ret[t, d] = v

    project(0, lambda cols: mm(hid[0], wd[:, cols]))

    share(1)
    shared(1)

    def down_step(j, carry):
        cols = pl.ds(pl.multiple_of(j * tile, tile), tile)
        hdy = mm(slots[0, 1].reshape(rows, half), wd[cols, pl.ds(0, half)], TRAIL) + mm(
            slots[1, 1].reshape(rows, half), wd[cols, pl.ds(half, half)], TRAIL
        )
        g = gpre[:, cols]
        sig = jax.nn.sigmoid(g)
        hid[1, :, cols] = (hdy * upre[:, cols] * sig * (1.0 + g * (1.0 - sig))).astype(BF16)
        hid[2, :, cols] = (hdy * (g * sig)).astype(BF16)
        return carry

    lax.fori_loop(0, units // tile, down_step, 0)
    stores = [
        pltpu.make_async_copy(slots, slots_hbm, o_sem.at[0]),
        pltpu.make_async_copy(hid, hidden_hbm, o_sem.at[1]),
    ]
    for cp in stores:
        cp.start()

    project(1, lambda cols: mm(hid[1], wg[cols, :], TRAIL) + mm(hid[2], wu[cols, :], TRAIL))

    span = toks // nz

    def combine(t):
        for m in order:
            b = flip(d, m)
            remote(
                ret_snd.at[t, b], ret.at[t, b], r_send.at[t, m], r_recv.at[t, m], (b, f)
            ).wait_recv()
        flat = ret[t].reshape(rows, half)
        if t == 0:
            v = rweight[:, 0:1] * mm(first, flat, LEAD) + rweight[:, 1:2] * mm(second, flat, LEAD)
        else:
            v = mm(picked, flat, LEAD)
        zacc[t] = v.reshape(nz, span, half)

    def pieces(s, who):
        step = bits[s] * 2
        return [who % step + step * q for q in range(nz // step)]

    base = [sum(nz // (2 * b) for b in bits[:s]) for s in range(len(bits))]

    def reduce_start(t, s):
        zz = flip(z, bits[s])
        dev = (d, flip(f, 2 * bits[s]))
        cps = []
        for q, p in enumerate(pieces(s, zz)):
            k = base[s] + q
            zsnd[t, k] = zacc[t, p].astype(BF16)
            cp = remote(zsnd.at[t, k], zrcv.at[t, k], z_send.at[t, k], z_recv.at[t, k], dev)
            cp.start()
            cps.append(cp)
        sends.extend(cps)
        return cps

    def reduce_end(t, s, cps):
        for q, p in enumerate(pieces(s, z)):
            cps[q].wait_recv()
            zacc[t, p] += zrcv[t, base[s] + q].astype(F32)

    def spread_start(t, s):
        dev = (d, flip(f, 2 * bits[s]))
        cps = []
        for q, p in enumerate(pieces(s, z)):
            k = base[s] + q
            cp = remote(fin.at[c, t, p], fin.at[c, t, p], g_send.at[t, k], g_recv.at[t, k], dev)
            cp.start()
            cps.append(cp)
        sends.extend(cps)
        return None

    def spread_end(t, s, cps):
        dev = (d, flip(f, 2 * bits[s]))
        for q, p in enumerate(pieces(s, flip(z, bits[s]))):
            k = base[s] + q
            remote(
                fin.at[c, t, p], fin.at[c, t, p], g_send.at[t, k], g_recv.at[t, k], dev
            ).wait_recv()

    stages = [(reduce_start, reduce_end, s) for s in range(len(bits))]
    stages += [(spread_start, spread_end, s) for s in reversed(range(len(bits)))]

    def begin(t, i):
        if i == len(bits):
            fin[c, t, z] = zacc[t, z].astype(BF16)
        go, _, s = stages[i]
        return go(t, s)

    def last(t):
        cp = remote(fin.at[c, t], fin.at[c, t], h_send.at[t], h_recv.at[t], sib)
        cp.start()
        sends.append(cp)

    combine(0)
    flying = {0: begin(0, 0)}
    combine(1)
    flying[1] = begin(1, 0)
    for i in range(len(stages)):
        for t in range(2):
            _, end, s = stages[i]
            end(t, s, flying[t])
            if i + 1 < len(stages):
                flying[t] = begin(t, i + 1)
            else:
                last(t)

    for t, result in enumerate((output, input_grad)):
        remote(
            fin.at[1 - c, t], fin.at[1 - c, t], h_send.at[t], h_recv.at[t], sib
        ).wait_recv()
        for h in range(2):
            result[:, h * half : (h + 1) * half] = fin[h, t].reshape(toks, half)
    for cp in sends:
        cp.wait_send()
    for cp in stores:
        cp.wait()


def grads_kernel(x, dy, hid, grad_gate, grad_up, grad_down):
    rows = hid.shape[1]
    xt = x[0, 0].reshape(rows, x.shape[-1])
    dyt = dy[0, 0].reshape(rows, dy.shape[-1])
    grad_gate[...] = mm(xt, hid[1], LEAD).astype(BF16)
    grad_up[...] = mm(xt, hid[2], LEAD).astype(BF16)
    grad_down[...] = mm(hid[0], dyt, LEAD).astype(BF16)


def fused(tokens, cotangent, routes, router_weight, w_gate, w_up, w_down):
    n = lax.axis_size("dp")
    nz = lax.axis_size("fsdp") // 2
    toks, features = tokens.shape
    cap = capacity_of(toks, n)
    rows = n * cap
    half = features // 2
    units = w_gate.shape[2]
    tile = 256
    span = toks // nz
    vmem = pl.BlockSpec(memory_space=pltpu.VMEM)
    hbm = pl.BlockSpec(memory_space=pl.ANY)
    dma = pltpu.SemaphoreType.DMA
    V = pltpu.VMEM
    output, input_grad, slots, hid = pl.pallas_call(
        functools.partial(routed_kernel, n, nz, cap, tile),
        out_shape=(
            jax.ShapeDtypeStruct((toks, features), BF16),
            jax.ShapeDtypeStruct((toks, features), BF16),
            jax.ShapeDtypeStruct((2, 2, n, cap, half), BF16),
            jax.ShapeDtypeStruct((3, rows, units), BF16),
        ),
        in_specs=[vmem] * 5 + [hbm] * 3,
        out_specs=(vmem, vmem, hbm, hbm),
        scratch_shapes=[
            V((features, units), BF16),
            V((features, units), BF16),
            V((units, features), BF16),
            V((2, 2, n, cap, half), BF16),
            V((2, n, cap, half), BF16),
            V((rows, units), F32),
            V((rows, units), F32),
            V((3, rows, units), BF16),
            V((2, n, cap, half), BF16),
            V((2, n, cap, half), BF16),
            V((2, rows, half), F32),
            V((2, n, cap, half), BF16),
            V((2, n, cap, half), BF16),
            V((2, nz, span, half), F32),
            V((2, nz, span, half), BF16),
            V((2, nz, span, half), BF16),
            V((2, 2, nz, span, half), BF16),
            dma((3,)),
            dma((2, n)), dma((2, n)), dma((2, n)), dma((2, n)),
            dma((2,)), dma((2,)),
            dma((2, n)), dma((2, n)),
            dma((2, nz)), dma((2, nz)), dma((2, nz)), dma((2, nz)),
            dma((2,)), dma((2,)),
            dma((2,)),
        ],
        compiler_params=pltpu.CompilerParams(
            collective_id=0, has_side_effects=True, vmem_limit_bytes=64 * 1000 * 1000
        ),
        name="routed",
    )(tokens, cotangent, routes.T, router_weight.T, router_weight, w_gate[0], w_up[0], w_down[0])

    wide = 512 if half % 512 == 0 else 128
    per = half // wide

    def slot_spec(t):
        return pl.BlockSpec((1, 1, n, cap, wide), lambda i: (i // per, t, 0, 0, i % per))

    grad_gate, grad_up, grad_down = pl.pallas_call(
        grads_kernel,
        grid=(features // wide,),
        out_shape=(
            jax.ShapeDtypeStruct((features, units), BF16),
            jax.ShapeDtypeStruct((features, units), BF16),
            jax.ShapeDtypeStruct((units, features), BF16),
        ),
        in_specs=[
            slot_spec(0),
            slot_spec(1),
            pl.BlockSpec((3, rows, units), lambda i: (0, 0, 0)),
        ],
        out_specs=(
            pl.BlockSpec((wide, units), lambda i: (i, 0)),
            pl.BlockSpec((wide, units), lambda i: (i, 0)),
            pl.BlockSpec((units, wide), lambda i: (0, i)),
        ),
        compiler_params=pltpu.CompilerParams(vmem_limit_bytes=60 * 1000 * 1000),
        name="grads",
    )(slots, slots, hid)
    return output, input_grad, grad_gate[None], grad_up[None], grad_down[None]


def slot_tables(routes, router_weight, experts, capacity):
    expert_ids = jnp.arange(experts, dtype=jnp.int32)
    hit_table = (routes[:, :, None] == expert_ids).astype(jnp.int32)
    per_token = jnp.sum(hit_table, axis=1)
    before = jnp.cumsum(per_token, axis=0) - per_token
    slot_of = jnp.sum(hit_table * before[:, None, :], axis=2)
    slot_ids = jnp.arange(capacity, dtype=jnp.int32)
    placed = hit_table[:, :, :, None] * (slot_of[:, :, None, None] == slot_ids).astype(jnp.int32)
    tok_rows = routes.shape[0]
    flat = placed.reshape(tok_rows, 2, experts * capacity).astype(jnp.float32)
    slot_weight = jnp.sum(flat * router_weight[:, :, None], axis=(0, 1))
    return (flat[:, 0], flat[:, 1], slot_weight)


def on_device(tokens, cotangent, routes, router_weight, w_gate, w_up, w_down):
    experts = lax.axis_size("dp")
    tok_rows, features = tokens.shape
    capacity = max(tok_rows * 3 // 8, tok_rows * 2 // experts, 2)
    local_rows = experts * capacity
    lead = (((0,), (0,)), ((), ()))
    trail = (((1,), (1,)), ((), ()))
    first_pick, second_pick, slot_weight = slot_tables(routes, router_weight, experts, capacity)
    picked = (first_pick + second_pick).astype(jnp.bfloat16)
    send_x = lax.dot_general(picked, tokens, lead, preferred_element_type=jnp.float32).astype(
        jnp.bfloat16
    )
    chosen_dy = lax.dot_general(picked, cotangent, lead, preferred_element_type=jnp.float32)
    send_dy = (chosen_dy * slot_weight[:, None]).astype(jnp.bfloat16)
    arrived_x, arrived_dy = (
        lax.all_to_all(
            send_x.reshape(experts, capacity, features),
            "dp",
            split_axis=0,
            concat_axis=0,
            tiled=True,
        ),
        lax.all_to_all(
            send_dy.reshape(experts, capacity, features),
            "dp",
            split_axis=0,
            concat_axis=0,
            tiled=True,
        ),
    )
    slot_x = arrived_x.reshape(local_rows, features)
    slot_dy = arrived_dy.reshape(local_rows, features)
    gate_w = w_gate[0]
    up_w = w_up[0]
    down_w = w_down[0]
    gate_pre = jnp.dot(slot_x, gate_w, preferred_element_type=jnp.float32)
    up_pre = jnp.dot(slot_x, up_w, preferred_element_type=jnp.float32)
    sigma = jax.nn.sigmoid(gate_pre)
    active = gate_pre * sigma
    hidden = (active * up_pre).astype(jnp.bfloat16)
    out_terms = jnp.dot(hidden, down_w, preferred_element_type=jnp.float32)
    hidden_dy = lax.dot_general(slot_dy, down_w, trail, preferred_element_type=jnp.float32)
    gate_dy = (hidden_dy * up_pre * sigma * (1.0 + gate_pre * (1.0 - sigma))).astype(jnp.bfloat16)
    up_dy = (hidden_dy * active).astype(jnp.bfloat16)
    grad_down = lax.dot_general(hidden, slot_dy, lead, preferred_element_type=jnp.float32).astype(
        jnp.bfloat16
    )
    grad_gate = lax.dot_general(slot_x, gate_dy, lead, preferred_element_type=jnp.float32).astype(
        jnp.bfloat16
    )
    grad_up = lax.dot_general(slot_x, up_dy, lead, preferred_element_type=jnp.float32).astype(
        jnp.bfloat16
    )
    back_terms = lax.dot_general(
        gate_dy, gate_w, trail, preferred_element_type=jnp.float32
    ) + lax.dot_general(up_dy, up_w, trail, preferred_element_type=jnp.float32)
    out_part, back_part = (
        lax.psum_scatter(
            out_terms.reshape(experts, capacity, features).astype(jnp.bfloat16),
            "fsdp",
            scatter_dimension=2,
            tiled=True,
        ).astype(jnp.float32),
        lax.psum_scatter(
            back_terms.reshape(experts, capacity, features).astype(jnp.bfloat16),
            "fsdp",
            scatter_dimension=2,
            tiled=True,
        ).astype(jnp.float32),
    )
    returned_out, returned_dx = (
        lax.all_to_all(
            out_part.astype(jnp.bfloat16), "dp", split_axis=0, concat_axis=0, tiled=True
        ),
        lax.all_to_all(
            back_part.astype(jnp.bfloat16), "dp", split_axis=0, concat_axis=0, tiled=True
        ),
    )
    width = out_part.shape[2]
    flat_out = returned_out.reshape(local_rows, width)
    flat_dx = returned_dx.reshape(local_rows, width)
    first_rows = jnp.dot(
        first_pick.astype(jnp.bfloat16), flat_out, preferred_element_type=jnp.float32
    )
    second_rows = jnp.dot(
        second_pick.astype(jnp.bfloat16), flat_out, preferred_element_type=jnp.float32
    )
    output = (router_weight[:, 0:1] * first_rows + router_weight[:, 1:2] * second_rows).astype(
        jnp.bfloat16
    )
    input_grad = jnp.dot(picked, flat_dx, preferred_element_type=jnp.float32).astype(jnp.bfloat16)
    output, input_grad = (
        lax.all_gather(output, "fsdp", axis=1, tiled=True),
        lax.all_gather(input_grad, "fsdp", axis=1, tiled=True),
    )
    return (output, input_grad, grad_gate[None], grad_up[None], grad_down[None])


def capacity_of(toks, experts):
    return max(toks * 3 // 8, toks * 2 // experts, 2)


def fits(mesh, toks, features, units):
    n, m = mesh.shape["dp"], mesh.shape["fsdp"]
    cap = capacity_of(toks, n)
    powers = n & (n - 1) == 0 and m & (m - 1) == 0 and m >= 4
    whole = features % 512 == 0 and units % 256 == 0 and cap % 16 == 0 and toks % (8 * m) == 0
    rows = n * cap
    held = 6 * features * units + 2 * rows * (13 * features + 7 * units) + 20 * toks * features
    return powers and whole and held < 56 * 1000 * 1000


def solution(mesh):
    def step(tokens, cotangent, routes, router_weight, w_gate, w_up, w_down):
        body = fused if fits(mesh, *tokens.shape, w_gate.shape[2]) else on_device
        return body(tokens, cotangent, routes, router_weight, w_gate, w_up, w_down)

    return jax.shard_map(
        step,
        mesh=mesh,
        in_specs=(
            P("dp", None),
            P("dp", None),
            P("dp", None),
            P("dp", None),
            P("dp", None, "fsdp"),
            P("dp", None, "fsdp"),
            P("dp", "fsdp", None),
        ),
        out_specs=(
            P("dp", None),
            P("dp", None),
            P("dp", None, "fsdp"),
            P("dp", None, "fsdp"),
            P("dp", "fsdp", None),
        ),
        check_vma=False,
    )
```

```python
import functools

import jax
import jax.numpy as jnp
from jax import lax
from jax.experimental import pallas as pl
from jax.experimental.pallas import tpu as pltpu
from jax.sharding import PartitionSpec as P

MESH = pl.DeviceIdType.MESH
BF16 = jnp.bfloat16
F32 = jnp.float32
LEAD = (((0,), (0,)), ((), ()))
TRAIL = (((1,), (1,)), ((), ()))


def flip(a, mask):
    bit = 1
    while bit <= mask:
        if mask & bit:
            a = a + bit - 2 * bit * ((a // bit) % 2)
        bit *= 2
    return a


def mm(a, b, dims=(((1,), (0,)), ((), ()))):
    return lax.dot_general(a, b, dims, preferred_element_type=F32)


def routed_kernel(
    n, nz, cap, tile, chunks, lag,
    tokens, cotangent, routes_t, rweight_t, rweight, wg_hbm, wu_hbm, wd_hbm,
    output, input_grad, slots_hbm, hidden_hbm,
    wg, wu, wd, slots, snd, gpre, upre, hid,
    core_snd, core_rcv, own, ret_snd, ret, zacc, zsnd, zrcv, fin,
    w_sem, a_send, a_recv, f_send, f_recv, c_send, c_recv, r_send, r_recv,
    z_send, z_recv, g_send, g_recv, h_send, h_recv, o_sem,
):
    d = lax.axis_index("dp")
    f = lax.axis_index("fsdp")
    c = f % 2
    z = f // 2
    sib = (d, flip(f, 1))
    toks, features = tokens.shape
    half = features // 2
    width = half // chunks
    rows = n * cap
    units = hid.shape[2]
    order = sorted(range(1, n), key=lambda m: -bin(m).count("1"))
    bits = [1 << s for s in range(nz.bit_length() - 1)]

    def remote(src, dst, ssem, rsem, dev):
        return pltpu.make_async_remote_copy(
            src_ref=src, dst_ref=dst, send_sem=ssem, recv_sem=rsem,
            device_id=dev, device_id_type=MESH,
        )

    loads = [
        pltpu.make_async_copy(s, t, w_sem.at[k])
        for k, (s, t) in enumerate(((wg_hbm, wg), (wu_hbm, wu), (wd_hbm, wd)))
    ]
    for load in loads:
        load.start()

    barrier = pltpu.get_barrier_semaphore()
    friends = [(flip(d, m), f) for m in order] + [sib] + [(d, flip(f, 2 * b)) for b in bits]
    for dev in friends:
        pl.semaphore_signal(barrier, inc=1, device_id=dev, device_id_type=MESH)

    slot_row = lax.broadcasted_iota(jnp.int32, (rows, toks), 0)
    e_of = slot_row // cap
    s_of = (slot_row % cap).astype(F32)
    r = routes_t[...]
    hit0 = r[0:1, :] == e_of
    hit1 = r[1:2, :] == e_of
    per_token = jnp.where(hit0 | hit1, 1.0, 0.0).astype(BF16)
    earlier = (
        lax.broadcasted_iota(jnp.int32, (toks, toks), 0)
        < lax.broadcasted_iota(jnp.int32, (toks, toks), 1)
    )
    before = mm(per_token, jnp.where(earlier, 1.0, 0.0).astype(BF16))
    here = before == s_of
    first = jnp.where(hit0 & here, 1.0, 0.0)
    second = jnp.where(hit1 & here, 1.0, 0.0)
    rw = rweight_t[...]
    slot_weight = jnp.sum(first * rw[0:1, :] + second * rw[1:2, :], axis=1, keepdims=True)
    first = first.astype(BF16)
    second = second.astype(BF16)
    picked = first + second

    mine = pl.ds(pl.multiple_of(c * half, 128), half)
    snd[0] = mm(picked, tokens[:, mine]).astype(BF16).reshape(n, cap, half)
    pl.semaphore_wait(barrier, len(friends))

    sends = []

    def dispatch(t):
        for m in order:
            e = flip(d, m)
            cp = remote(snd.at[t, e], slots.at[c, t, d], a_send.at[t, m], a_recv.at[t, m], (e, f))
            cp.start()
            sends.append(cp)
        slots[c, t, d] = snd[t, d]

    def share(t):
        for m in [0] + order:
            b = flip(d, m)
            if m:
                remote(
                    snd.at[t, b], slots.at[c, t, b], a_send.at[t, m], a_recv.at[t, m], (b, f)
                ).wait_recv()
            cp = remote(slots.at[c, t, b], slots.at[c, t, b], f_send.at[t, m], f_recv.at[t, m], sib)
            cp.start()
            sends.append(cp)

    def shared(t):
        for m in [0] + order:
            b = flip(d, m)
            remote(
                slots.at[1 - c, t, b], slots.at[1 - c, t, b], f_send.at[t, m], f_recv.at[t, m], sib
            ).wait_recv()

    dispatch(0)
    snd[1] = (mm(picked, cotangent[:, mine]) * slot_weight).astype(BF16).reshape(n, cap, half)
    dispatch(1)
    share(0)
    shared(0)
    loads[0].wait()
    loads[1].wait()

    def up_step(j, carry):
        cols = pl.ds(pl.multiple_of(j * tile, tile), tile)
        x0 = slots[0, 0].reshape(rows, half)
        x1 = slots[1, 0].reshape(rows, half)
        g = mm(x0, wg[pl.ds(0, half), cols]) + mm(x1, wg[pl.ds(half, half), cols])
        u = mm(x0, wu[pl.ds(0, half), cols]) + mm(x1, wu[pl.ds(half, half), cols])
        gpre[:, cols] = g
        upre[:, cols] = u
        hid[0, :, cols] = (g * jax.nn.sigmoid(g) * u).astype(BF16)
        return carry

    lax.fori_loop(0, units // tile, up_step, 0)
    loads[2].wait()

    def project(t, term):
        def theirs(q, k, carry):
            cols = pl.ds(pl.multiple_of(k * tile, tile), tile)
            at = pl.multiple_of((1 - c) * half + q * width + k * tile, tile)
            v = term(pl.ds(at, tile))
            core_snd[t, q, :, :, cols] = v.astype(BF16).reshape(n, cap, tile)
            return carry

        def ours(q, k, carry):
            cols = pl.ds(pl.multiple_of(k * tile, tile), tile)
            at = pl.multiple_of(c * half + q * width + k * tile, tile)
            own[t, q, :, cols] = term(pl.ds(at, tile))
            return carry

        halves = []
        for q in range(chunks):
            lax.fori_loop(0, width // tile, functools.partial(theirs, q), 0)
            cp = remote(
                core_snd.at[t, q], core_rcv.at[t, q], c_send.at[t, q], c_recv.at[t, q], sib
            )
            cp.start()
            halves.append(cp)
        for q in range(chunks):
            lax.fori_loop(0, width // tile, functools.partial(ours, q), 0)
            halves[q].wait_recv()
            for m in order + [0]:
                b = flip(d, m)
                at = pl.ds(pl.multiple_of(b * cap, 16), cap)
                v = (own[t, q, at, :] + core_rcv[t, q, b].astype(F32)).astype(BF16)
                if m:
                    ret_snd[t, q, b] = v
                    cp = returned(t, q, m, b, d)
                    cp.start()
                    sends.append(cp)
                else:
                    ret[t, q, d] = v
        sends.extend(halves)

    def returned(t, q, m, b, where):
        return remote(
            ret_snd.at[t, q, b],
            ret.at[t, q, where],
            r_send.at[t, q, m],
            r_recv.at[t, q, m],
            (b, f),
        )

    project(0, lambda cols: mm(hid[0], wd[:, cols]))

    share(1)
    shared(1)

    def down_step(j, carry):
        cols = pl.ds(pl.multiple_of(j * tile, tile), tile)
        hdy = mm(slots[0, 1].reshape(rows, half), wd[cols, pl.ds(0, half)], TRAIL) + mm(
            slots[1, 1].reshape(rows, half), wd[cols, pl.ds(half, half)], TRAIL
        )
        g = gpre[:, cols]
        sig = jax.nn.sigmoid(g)
        hid[1, :, cols] = (hdy * upre[:, cols] * sig * (1.0 + g * (1.0 - sig))).astype(BF16)
        hid[2, :, cols] = (hdy * (g * sig)).astype(BF16)
        return carry

    lax.fori_loop(0, units // tile, down_step, 0)
    stores = [
        pltpu.make_async_copy(slots, slots_hbm, o_sem.at[0]),
        pltpu.make_async_copy(hid, hidden_hbm, o_sem.at[1]),
    ]
    for cp in stores:
        cp.start()

    project(1, lambda cols: mm(hid[1], wg[cols, :], TRAIL) + mm(hid[2], wu[cols, :], TRAIL))

    span = toks // nz

    def combine(t, q):
        for m in order:
            b = flip(d, m)
            returned(t, q, m, b, b).wait_recv()
        flat = ret[t, q].reshape(rows, width)
        if t == 0:
            v = rweight[:, 0:1] * mm(first, flat, LEAD) + rweight[:, 1:2] * mm(second, flat, LEAD)
        else:
            v = mm(picked, flat, LEAD)
        zacc[t, q] = v.reshape(nz, span, width)

    def pieces(s, who):
        step = bits[s] * 2
        return [who % step + step * q for q in range(nz // step)]

    base = [sum(nz // (2 * b) for b in bits[:s]) for s in range(len(bits))]

    def summing(t, q, s, k):
        dev = (d, flip(f, 2 * bits[s]))
        return remote(
            zsnd.at[t, q, k], zrcv.at[t, q, k], z_send.at[t, q, k], z_recv.at[t, q, k], dev
        )

    def spreading(t, q, s, k, p):
        dev = (d, flip(f, 2 * bits[s]))
        piece = fin.at[c, t, q, p]
        return remote(piece, piece, g_send.at[t, q, k], g_recv.at[t, q, k], dev)

    def reduce_start(t, q, s):
        for i, p in enumerate(pieces(s, flip(z, bits[s]))):
            k = base[s] + i
            zsnd[t, q, k] = zacc[t, q, p].astype(BF16)
            cp = summing(t, q, s, k)
            cp.start()
            sends.append(cp)

    def reduce_end(t, q, s):
        for i, p in enumerate(pieces(s, z)):
            k = base[s] + i
            summing(t, q, s, k).wait_recv()
            zacc[t, q, p] += zrcv[t, q, k].astype(F32)

    def spread_start(t, q, s):
        for i, p in enumerate(pieces(s, z)):
            cp = spreading(t, q, s, base[s] + i, p)
            cp.start()
            sends.append(cp)

    def spread_end(t, q, s):
        for i, p in enumerate(pieces(s, flip(z, bits[s]))):
            spreading(t, q, s, base[s] + i, p).wait_recv()

    def last(t, q, h):
        piece = fin.at[h, t, q]
        return remote(piece, piece, h_send.at[t, q], h_recv.at[t, q], sib)

    stages = [(reduce_start, reduce_end, s) for s in range(len(bits))]
    stages += [(spread_start, spread_end, s) for s in reversed(range(len(bits)))]

    def advance(t, q, i):
        if i == 0:
            combine(t, q)
        else:
            _, end, s = stages[i - 1]
            end(t, q, s)
        if i == len(bits):
            fin[c, t, q, z] = zacc[t, q, z].astype(BF16)
        if i < len(stages):
            begin, _, s = stages[i]
            begin(t, q, s)
        else:
            cp = last(t, q, c)
            cp.start()
            sends.append(cp)

    todo = [
        (i + lag * t, t, q, i) for i in range(len(stages) + 1) for t in range(2) for q in range(chunks)
    ]
    for _, t, q, i in sorted(todo):
        advance(t, q, i)

    for t, result in enumerate((output, input_grad)):
        for q in range(chunks):
            last(t, q, 1 - c).wait_recv()
            for h in range(2):
                at = h * half + q * width
                result[:, at : at + width] = fin[h, t, q].reshape(toks, width)
    for cp in sends:
        cp.wait_send()
    for cp in stores:
        cp.wait()


def grads_kernel(x, dy, hid, grad_gate, grad_up, grad_down):
    rows = hid.shape[1]
    xt = x[0, 0].reshape(rows, x.shape[-1])
    dyt = dy[0, 0].reshape(rows, dy.shape[-1])
    grad_gate[...] = mm(xt, hid[1], LEAD).astype(BF16)
    grad_up[...] = mm(xt, hid[2], LEAD).astype(BF16)
    grad_down[...] = mm(hid[0], dyt, LEAD).astype(BF16)


def fused(tokens, cotangent, routes, router_weight, w_gate, w_up, w_down):
    n = lax.axis_size("dp")
    nz = lax.axis_size("fsdp") // 2
    toks, features = tokens.shape
    cap = capacity_of(toks, n)
    rows = n * cap
    half = features // 2
    units = w_gate.shape[2]
    tile = 256
    chunks = 2
    width = half // chunks
    span = toks // nz
    vmem = pl.BlockSpec(memory_space=pltpu.VMEM)
    hbm = pl.BlockSpec(memory_space=pl.ANY)
    dma = pltpu.SemaphoreType.DMA
    V = pltpu.VMEM
    output, input_grad, slots, hid = pl.pallas_call(
        functools.partial(routed_kernel, n, nz, cap, tile, chunks, 2),
        out_shape=(
            jax.ShapeDtypeStruct((toks, features), BF16),
            jax.ShapeDtypeStruct((toks, features), BF16),
            jax.ShapeDtypeStruct((2, 2, n, cap, half), BF16),
            jax.ShapeDtypeStruct((3, rows, units), BF16),
        ),
        in_specs=[vmem] * 5 + [hbm] * 3,
        out_specs=(vmem, vmem, hbm, hbm),
        scratch_shapes=[
            V((features, units), BF16),
            V((features, units), BF16),
            V((units, features), BF16),
            V((2, 2, n, cap, half), BF16),
            V((2, n, cap, half), BF16),
            V((rows, units), F32),
            V((rows, units), F32),
            V((3, rows, units), BF16),
            V((2, chunks, n, cap, width), BF16),
            V((2, chunks, n, cap, width), BF16),
            V((2, chunks, rows, width), F32),
            V((2, chunks, n, cap, width), BF16),
            V((2, chunks, n, cap, width), BF16),
            V((2, chunks, nz, span, width), F32),
            V((2, chunks, nz, span, width), BF16),
            V((2, chunks, nz, span, width), BF16),
            V((2, 2, chunks, nz, span, width), BF16),
            dma((3,)),
            dma((2, n)), dma((2, n)), dma((2, n)), dma((2, n)),
            dma((2, chunks)), dma((2, chunks)),
            dma((2, chunks, n)), dma((2, chunks, n)),
            dma((2, chunks, nz)), dma((2, chunks, nz)), dma((2, chunks, nz)), dma((2, chunks, nz)),
            dma((2, chunks)), dma((2, chunks)),
            dma((2,)),
        ],
        compiler_params=pltpu.CompilerParams(
            collective_id=0, has_side_effects=True, vmem_limit_bytes=64 * 1000 * 1000
        ),
        name="routed",
    )(tokens, cotangent, routes.T, router_weight.T, router_weight, w_gate[0], w_up[0], w_down[0])

    wide = 512 if half % 512 == 0 else 128
    per = half // wide

    def slot_spec(t):
        return pl.BlockSpec((1, 1, n, cap, wide), lambda i: (i // per, t, 0, 0, i % per))

    grad_gate, grad_up, grad_down = pl.pallas_call(
        grads_kernel,
        grid=(features // wide,),
        out_shape=(
            jax.ShapeDtypeStruct((features, units), BF16),
            jax.ShapeDtypeStruct((features, units), BF16),
            jax.ShapeDtypeStruct((units, features), BF16),
        ),
        in_specs=[
            slot_spec(0),
            slot_spec(1),
            pl.BlockSpec((3, rows, units), lambda i: (0, 0, 0)),
        ],
        out_specs=(
            pl.BlockSpec((wide, units), lambda i: (i, 0)),
            pl.BlockSpec((wide, units), lambda i: (i, 0)),
            pl.BlockSpec((units, wide), lambda i: (0, i)),
        ),
        compiler_params=pltpu.CompilerParams(vmem_limit_bytes=60 * 1000 * 1000),
        name="grads",
    )(slots, slots, hid)
    return output, input_grad, grad_gate[None], grad_up[None], grad_down[None]


def slot_tables(routes, router_weight, experts, capacity):
    expert_ids = jnp.arange(experts, dtype=jnp.int32)
    hit_table = (routes[:, :, None] == expert_ids).astype(jnp.int32)
    per_token = jnp.sum(hit_table, axis=1)
    before = jnp.cumsum(per_token, axis=0) - per_token
    slot_of = jnp.sum(hit_table * before[:, None, :], axis=2)
    slot_ids = jnp.arange(capacity, dtype=jnp.int32)
    placed = hit_table[:, :, :, None] * (slot_of[:, :, None, None] == slot_ids).astype(jnp.int32)
    tok_rows = routes.shape[0]
    flat = placed.reshape(tok_rows, 2, experts * capacity).astype(jnp.float32)
    slot_weight = jnp.sum(flat * router_weight[:, :, None], axis=(0, 1))
    return (flat[:, 0], flat[:, 1], slot_weight)


def on_device(tokens, cotangent, routes, router_weight, w_gate, w_up, w_down):
    experts = lax.axis_size("dp")
    tok_rows, features = tokens.shape
    capacity = max(tok_rows * 3 // 8, tok_rows * 2 // experts, 2)
    local_rows = experts * capacity
    lead = (((0,), (0,)), ((), ()))
    trail = (((1,), (1,)), ((), ()))
    first_pick, second_pick, slot_weight = slot_tables(routes, router_weight, experts, capacity)
    picked = (first_pick + second_pick).astype(jnp.bfloat16)
    send_x = lax.dot_general(picked, tokens, lead, preferred_element_type=jnp.float32).astype(
        jnp.bfloat16
    )
    chosen_dy = lax.dot_general(picked, cotangent, lead, preferred_element_type=jnp.float32)
    send_dy = (chosen_dy * slot_weight[:, None]).astype(jnp.bfloat16)
    arrived_x, arrived_dy = (
        lax.all_to_all(
            send_x.reshape(experts, capacity, features),
            "dp",
            split_axis=0,
            concat_axis=0,
            tiled=True,
        ),
        lax.all_to_all(
            send_dy.reshape(experts, capacity, features),
            "dp",
            split_axis=0,
            concat_axis=0,
            tiled=True,
        ),
    )
    slot_x = arrived_x.reshape(local_rows, features)
    slot_dy = arrived_dy.reshape(local_rows, features)
    gate_w = w_gate[0]
    up_w = w_up[0]
    down_w = w_down[0]
    gate_pre = jnp.dot(slot_x, gate_w, preferred_element_type=jnp.float32)
    up_pre = jnp.dot(slot_x, up_w, preferred_element_type=jnp.float32)
    sigma = jax.nn.sigmoid(gate_pre)
    active = gate_pre * sigma
    hidden = (active * up_pre).astype(jnp.bfloat16)
    out_terms = jnp.dot(hidden, down_w, preferred_element_type=jnp.float32)
    hidden_dy = lax.dot_general(slot_dy, down_w, trail, preferred_element_type=jnp.float32)
    gate_dy = (hidden_dy * up_pre * sigma * (1.0 + gate_pre * (1.0 - sigma))).astype(jnp.bfloat16)
    up_dy = (hidden_dy * active).astype(jnp.bfloat16)
    grad_down = lax.dot_general(hidden, slot_dy, lead, preferred_element_type=jnp.float32).astype(
        jnp.bfloat16
    )
    grad_gate = lax.dot_general(slot_x, gate_dy, lead, preferred_element_type=jnp.float32).astype(
        jnp.bfloat16
    )
    grad_up = lax.dot_general(slot_x, up_dy, lead, preferred_element_type=jnp.float32).astype(
        jnp.bfloat16
    )
    back_terms = lax.dot_general(
        gate_dy, gate_w, trail, preferred_element_type=jnp.float32
    ) + lax.dot_general(up_dy, up_w, trail, preferred_element_type=jnp.float32)
    out_part, back_part = (
        lax.psum_scatter(
            out_terms.reshape(experts, capacity, features).astype(jnp.bfloat16),
            "fsdp",
            scatter_dimension=2,
            tiled=True,
        ).astype(jnp.float32),
        lax.psum_scatter(
            back_terms.reshape(experts, capacity, features).astype(jnp.bfloat16),
            "fsdp",
            scatter_dimension=2,
            tiled=True,
        ).astype(jnp.float32),
    )
    returned_out, returned_dx = (
        lax.all_to_all(
            out_part.astype(jnp.bfloat16), "dp", split_axis=0, concat_axis=0, tiled=True
        ),
        lax.all_to_all(
            back_part.astype(jnp.bfloat16), "dp", split_axis=0, concat_axis=0, tiled=True
        ),
    )
    width = out_part.shape[2]
    flat_out = returned_out.reshape(local_rows, width)
    flat_dx = returned_dx.reshape(local_rows, width)
    first_rows = jnp.dot(
        first_pick.astype(jnp.bfloat16), flat_out, preferred_element_type=jnp.float32
    )
    second_rows = jnp.dot(
        second_pick.astype(jnp.bfloat16), flat_out, preferred_element_type=jnp.float32
    )
    output = (router_weight[:, 0:1] * first_rows + router_weight[:, 1:2] * second_rows).astype(
        jnp.bfloat16
    )
    input_grad = jnp.dot(picked, flat_dx, preferred_element_type=jnp.float32).astype(jnp.bfloat16)
    output, input_grad = (
        lax.all_gather(output, "fsdp", axis=1, tiled=True),
        lax.all_gather(input_grad, "fsdp", axis=1, tiled=True),
    )
    return (output, input_grad, grad_gate[None], grad_up[None], grad_down[None])


def capacity_of(toks, experts):
    return max(toks * 3 // 8, toks * 2 // experts, 2)


def fits(mesh, toks, features, units):
    n, m = mesh.shape["dp"], mesh.shape["fsdp"]
    cap = capacity_of(toks, n)
    powers = n & (n - 1) == 0 and m & (m - 1) == 0 and m >= 4
    whole = features % 1024 == 0 and units % 256 == 0 and cap % 16 == 0 and toks % (8 * m) == 0
    rows = n * cap
    held = 6 * features * units + 2 * rows * (13 * features + 7 * units) + 20 * toks * features
    return powers and whole and held < 56 * 1000 * 1000


def solution(mesh):
    def step(tokens, cotangent, routes, router_weight, w_gate, w_up, w_down):
        body = fused if fits(mesh, *tokens.shape, w_gate.shape[2]) else on_device
        return body(tokens, cotangent, routes, router_weight, w_gate, w_up, w_down)

    return jax.shard_map(
        step,
        mesh=mesh,
        in_specs=(
            P("dp", None),
            P("dp", None),
            P("dp", None),
            P("dp", None),
            P("dp", None, "fsdp"),
            P("dp", None, "fsdp"),
            P("dp", "fsdp", None),
        ),
        out_specs=(
            P("dp", None),
            P("dp", None),
            P("dp", None, "fsdp"),
            P("dp", None, "fsdp"),
            P("dp", "fsdp", None),
        ),
        check_vma=False,
    )
```

```python
import functools

import jax
import jax.numpy as jnp
from jax import lax
from jax.experimental import pallas as pl
from jax.experimental.pallas import tpu as pltpu
from jax.sharding import PartitionSpec as P

MESH = pl.DeviceIdType.MESH
BF16 = jnp.bfloat16
F32 = jnp.float32
LEAD = (((0,), (0,)), ((), ()))
TRAIL = (((1,), (1,)), ((), ()))


def flip(a, mask):
    bit = 1
    while bit <= mask:
        if mask & bit:
            a = a + bit - 2 * bit * ((a // bit) % 2)
        bit *= 2
    return a


def mm(a, b, dims=(((1,), (0,)), ((), ()))):
    return lax.dot_general(a, b, dims, preferred_element_type=F32)


def routed_kernel(
    n, nz, cap, tile, chunks, lag,
    tokens, cotangent, routes_t, rweight_t, rweight, wg_hbm, wu_hbm, wd_hbm,
    output, input_grad, slots_hbm, hidden_hbm,
    wg, wu, wd, slots, snd, gpre, upre, hid,
    core_snd, core_rcv, own, ret_snd, ret, zacc, zsnd, zrcv, fin,
    w_sem, a_send, a_recv, f_send, f_recv, c_send, c_recv, r_send, r_recv,
    z_send, z_recv, g_send, g_recv, h_send, h_recv, o_sem,
):
    d = lax.axis_index("dp")
    f = lax.axis_index("fsdp")
    c = f % 2
    z = f // 2
    sib = (d, flip(f, 1))
    toks, features = tokens.shape
    half = features // 2
    width = half // chunks
    rows = n * cap
    units = hid.shape[2]
    order = sorted(range(1, n), key=lambda m: -bin(m).count("1"))
    bits = [1 << s for s in range(nz.bit_length() - 1)]

    def remote(src, dst, ssem, rsem, dev):
        return pltpu.make_async_remote_copy(
            src_ref=src, dst_ref=dst, send_sem=ssem, recv_sem=rsem,
            device_id=dev, device_id_type=MESH,
        )

    loads = [
        pltpu.make_async_copy(s, t, w_sem.at[k])
        for k, (s, t) in enumerate(((wg_hbm, wg), (wu_hbm, wu), (wd_hbm, wd)))
    ]
    for load in loads:
        load.start()

    barrier = pltpu.get_barrier_semaphore()
    friends = [(flip(d, m), f) for m in order] + [sib] + [(d, flip(f, 2 * b)) for b in bits]
    for dev in friends:
        pl.semaphore_signal(barrier, inc=1, device_id=dev, device_id_type=MESH)

    slot_row = lax.broadcasted_iota(jnp.int32, (rows, toks), 0)
    e_of = slot_row // cap
    s_of = (slot_row % cap).astype(F32)
    r = routes_t[...]
    hit0 = r[0:1, :] == e_of
    hit1 = r[1:2, :] == e_of
    per_token = jnp.where(hit0 | hit1, 1.0, 0.0).astype(BF16)
    earlier = (
        lax.broadcasted_iota(jnp.int32, (toks, toks), 0)
        < lax.broadcasted_iota(jnp.int32, (toks, toks), 1)
    )
    before = mm(per_token, jnp.where(earlier, 1.0, 0.0).astype(BF16))
    here = before == s_of
    first = jnp.where(hit0 & here, 1.0, 0.0)
    second = jnp.where(hit1 & here, 1.0, 0.0)
    rw = rweight_t[...]
    slot_weight = jnp.sum(first * rw[0:1, :] + second * rw[1:2, :], axis=1, keepdims=True)
    first = first.astype(BF16)
    second = second.astype(BF16)
    picked = first + second

    mine = pl.ds(pl.multiple_of(c * half, 128), half)
    snd[0] = mm(picked, tokens[:, mine]).astype(BF16).reshape(n, cap, half)
    pl.semaphore_wait(barrier, len(friends))

    sends = []

    def dispatch(t):
        for m in order:
            e = flip(d, m)
            cp = remote(snd.at[t, e], slots.at[c, t, d], a_send.at[t, m], a_recv.at[t, m], (e, f))
            cp.start()
            sends.append(cp)
        slots[c, t, d] = snd[t, d]

    def share(t):
        for m in [0] + order:
            b = flip(d, m)
            if m:
                remote(
                    snd.at[t, b], slots.at[c, t, b], a_send.at[t, m], a_recv.at[t, m], (b, f)
                ).wait_recv()
            cp = remote(slots.at[c, t, b], slots.at[c, t, b], f_send.at[t, m], f_recv.at[t, m], sib)
            cp.start()
            sends.append(cp)

    def shared(t):
        for m in [0] + order:
            b = flip(d, m)
            remote(
                slots.at[1 - c, t, b], slots.at[1 - c, t, b], f_send.at[t, m], f_recv.at[t, m], sib
            ).wait_recv()

    dispatch(0)
    snd[1] = (mm(picked, cotangent[:, mine]) * slot_weight).astype(BF16).reshape(n, cap, half)
    dispatch(1)
    share(0)
    shared(0)
    loads[0].wait()
    loads[1].wait()

    def up_step(j, carry):
        cols = pl.ds(pl.multiple_of(j * tile, tile), tile)
        x0 = slots[0, 0].reshape(rows, half)
        x1 = slots[1, 0].reshape(rows, half)
        g = mm(x0, wg[pl.ds(0, half), cols]) + mm(x1, wg[pl.ds(half, half), cols])
        u = mm(x0, wu[pl.ds(0, half), cols]) + mm(x1, wu[pl.ds(half, half), cols])
        gpre[:, cols] = g
        upre[:, cols] = u
        hid[0, :, cols] = (g * jax.nn.sigmoid(g) * u).astype(BF16)
        return carry

    lax.fori_loop(0, units // tile, up_step, 0)
    loads[2].wait()

    def project(t, term):
        def theirs(q, k, carry):
            cols = pl.ds(pl.multiple_of(k * tile, tile), tile)
            at = pl.multiple_of((1 - c) * half + q * width + k * tile, tile)
            v = term(pl.ds(at, tile))
            core_snd[t, q, :, :, cols] = v.astype(BF16).reshape(n, cap, tile)
            return carry

        def ours(q, k, carry):
            cols = pl.ds(pl.multiple_of(k * tile, tile), tile)
            at = pl.multiple_of(c * half + q * width + k * tile, tile)
            own[t, q, :, cols] = term(pl.ds(at, tile))
            return carry

        halves = []
        for q in range(chunks):
            lax.fori_loop(0, width // tile, functools.partial(theirs, q), 0)
            cp = remote(
                core_snd.at[t, q], core_rcv.at[t, q], c_send.at[t, q], c_recv.at[t, q], sib
            )
            cp.start()
            halves.append(cp)
        for q in range(chunks):
            lax.fori_loop(0, width // tile, functools.partial(ours, q), 0)
            halves[q].wait_recv()
            for m in order + [0]:
                b = flip(d, m)
                at = pl.ds(pl.multiple_of(b * cap, 16), cap)
                v = (own[t, q, at, :] + core_rcv[t, q, b].astype(F32)).astype(BF16)
                if m:
                    ret_snd[t, q, b] = v
                    cp = returned(t, q, m, b, d)
                    cp.start()
                    sends.append(cp)
                else:
                    ret[t, q, d] = v
        sends.extend(halves)

    def returned(t, q, m, b, where):
        return remote(
            ret_snd.at[t, q, b],
            ret.at[t, q, where],
            r_send.at[t, q, m],
            r_recv.at[t, q, m],
            (b, f),
        )

    project(0, lambda cols: mm(hid[0], wd[:, cols]))

    share(1)
    shared(1)

    def down_step(j, carry):
        cols = pl.ds(pl.multiple_of(j * tile, tile), tile)
        hdy = mm(slots[0, 1].reshape(rows, half), wd[cols, pl.ds(0, half)], TRAIL) + mm(
            slots[1, 1].reshape(rows, half), wd[cols, pl.ds(half, half)], TRAIL
        )
        g = gpre[:, cols]
        sig = jax.nn.sigmoid(g)
        hid[1, :, cols] = (hdy * upre[:, cols] * sig * (1.0 + g * (1.0 - sig))).astype(BF16)
        hid[2, :, cols] = (hdy * (g * sig)).astype(BF16)
        return carry

    lax.fori_loop(0, units // tile, down_step, 0)
    stores = [
        pltpu.make_async_copy(slots, slots_hbm, o_sem.at[0]),
        pltpu.make_async_copy(hid, hidden_hbm, o_sem.at[1]),
    ]
    for cp in stores:
        cp.start()

    project(1, lambda cols: mm(hid[1], wg[cols, :], TRAIL) + mm(hid[2], wu[cols, :], TRAIL))

    span = toks // nz

    def combine(t, q):
        for m in order:
            b = flip(d, m)
            returned(t, q, m, b, b).wait_recv()
        flat = ret[t, q].reshape(rows, width)
        if t == 0:
            v = rweight[:, 0:1] * mm(first, flat, LEAD) + rweight[:, 1:2] * mm(second, flat, LEAD)
        else:
            v = mm(picked, flat, LEAD)
        zacc[t, q] = v.reshape(nz, span, width)

    def pieces(s, who):
        step = bits[s] * 2
        return [who % step + step * q for q in range(nz // step)]

    base = [sum(nz // (2 * b) for b in bits[:s]) for s in range(len(bits))]

    def summing(t, q, s, k):
        dev = (d, flip(f, 2 * bits[s]))
        return remote(
            zsnd.at[t, q, k], zrcv.at[t, q, k], z_send.at[t, q, k], z_recv.at[t, q, k], dev
        )

    def spreading(t, q, s, k, p):
        dev = (d, flip(f, 2 * bits[s]))
        piece = fin.at[c, t, q, p]
        return remote(piece, piece, g_send.at[t, q, k], g_recv.at[t, q, k], dev)

    def reduce_start(t, q, s):
        for i, p in enumerate(pieces(s, flip(z, bits[s]))):
            k = base[s] + i
            zsnd[t, q, k] = zacc[t, q, p].astype(BF16)
            cp = summing(t, q, s, k)
            cp.start()
            sends.append(cp)

    def reduce_end(t, q, s):
        for i, p in enumerate(pieces(s, z)):
            k = base[s] + i
            summing(t, q, s, k).wait_recv()
            zacc[t, q, p] += zrcv[t, q, k].astype(F32)

    def spread_start(t, q, s):
        for i, p in enumerate(pieces(s, z)):
            cp = spreading(t, q, s, base[s] + i, p)
            cp.start()
            sends.append(cp)

    def spread_end(t, q, s):
        for i, p in enumerate(pieces(s, flip(z, bits[s]))):
            spreading(t, q, s, base[s] + i, p).wait_recv()

    def last(t, q, h):
        piece = fin.at[h, t, q]
        return remote(piece, piece, h_send.at[t, q], h_recv.at[t, q], sib)

    stages = [(reduce_start, reduce_end, s) for s in range(len(bits))]
    stages += [(spread_start, spread_end, s) for s in reversed(range(len(bits)))]

    def advance(t, q, i):
        if i == 0:
            combine(t, q)
        else:
            _, end, s = stages[i - 1]
            end(t, q, s)
        if i == len(bits):
            fin[c, t, q, z] = zacc[t, q, z].astype(BF16)
        if i < len(stages):
            begin, _, s = stages[i]
            begin(t, q, s)
        else:
            cp = last(t, q, c)
            cp.start()
            sends.append(cp)

    todo = [
        (i + lag * t + 0.5 * q, t, q, i) for i in range(len(stages) + 1) for t in range(2) for q in range(chunks)
    ]
    for _, t, q, i in sorted(todo):
        advance(t, q, i)

    for t, result in enumerate((output, input_grad)):
        for q in range(chunks):
            last(t, q, 1 - c).wait_recv()
            for h in range(2):
                at = h * half + q * width
                result[:, at : at + width] = fin[h, t, q].reshape(toks, width)
    for cp in sends:
        cp.wait_send()
    for cp in stores:
        cp.wait()


def grads_kernel(x, dy, hid, grad_gate, grad_up, grad_down):
    rows = hid.shape[1]
    xt = x[0, 0].reshape(rows, x.shape[-1])
    dyt = dy[0, 0].reshape(rows, dy.shape[-1])
    grad_gate[...] = mm(xt, hid[1], LEAD).astype(BF16)
    grad_up[...] = mm(xt, hid[2], LEAD).astype(BF16)
    grad_down[...] = mm(hid[0], dyt, LEAD).astype(BF16)


def fused(tokens, cotangent, routes, router_weight, w_gate, w_up, w_down):
    n = lax.axis_size("dp")
    nz = lax.axis_size("fsdp") // 2
    toks, features = tokens.shape
    cap = capacity_of(toks, n)
    rows = n * cap
    half = features // 2
    units = w_gate.shape[2]
    tile = 256
    chunks = 2
    width = half // chunks
    span = toks // nz
    vmem = pl.BlockSpec(memory_space=pltpu.VMEM)
    hbm = pl.BlockSpec(memory_space=pl.ANY)
    dma = pltpu.SemaphoreType.DMA
    V = pltpu.VMEM
    output, input_grad, slots, hid = pl.pallas_call(
        functools.partial(routed_kernel, n, nz, cap, tile, chunks, 1),
        out_shape=(
            jax.ShapeDtypeStruct((toks, features), BF16),
            jax.ShapeDtypeStruct((toks, features), BF16),
            jax.ShapeDtypeStruct((2, 2, n, cap, half), BF16),
            jax.ShapeDtypeStruct((3, rows, units), BF16),
        ),
        in_specs=[vmem] * 5 + [hbm] * 3,
        out_specs=(vmem, vmem, hbm, hbm),
        scratch_shapes=[
            V((features, units), BF16),
            V((features, units), BF16),
            V((units, features), BF16),
            V((2, 2, n, cap, half), BF16),
            V((2, n, cap, half), BF16),
            V((rows, units), F32),
            V((rows, units), F32),
            V((3, rows, units), BF16),
            V((2, chunks, n, cap, width), BF16),
            V((2, chunks, n, cap, width), BF16),
            V((2, chunks, rows, width), F32),
            V((2, chunks, n, cap, width), BF16),
            V((2, chunks, n, cap, width), BF16),
            V((2, chunks, nz, span, width), F32),
            V((2, chunks, nz, span, width), BF16),
            V((2, chunks, nz, span, width), BF16),
            V((2, 2, chunks, nz, span, width), BF16),
            dma((3,)),
            dma((2, n)), dma((2, n)), dma((2, n)), dma((2, n)),
            dma((2, chunks)), dma((2, chunks)),
            dma((2, chunks, n)), dma((2, chunks, n)),
            dma((2, chunks, nz)), dma((2, chunks, nz)), dma((2, chunks, nz)), dma((2, chunks, nz)),
            dma((2, chunks)), dma((2, chunks)),
            dma((2,)),
        ],
        compiler_params=pltpu.CompilerParams(
            collective_id=0, has_side_effects=True, vmem_limit_bytes=64 * 1000 * 1000
        ),
        name="routed",
    )(tokens, cotangent, routes.T, router_weight.T, router_weight, w_gate[0], w_up[0], w_down[0])

    wide = 512 if half % 512 == 0 else 128
    per = half // wide

    def slot_spec(t):
        return pl.BlockSpec((1, 1, n, cap, wide), lambda i: (i // per, t, 0, 0, i % per))

    grad_gate, grad_up, grad_down = pl.pallas_call(
        grads_kernel,
        grid=(features // wide,),
        out_shape=(
            jax.ShapeDtypeStruct((features, units), BF16),
            jax.ShapeDtypeStruct((features, units), BF16),
            jax.ShapeDtypeStruct((units, features), BF16),
        ),
        in_specs=[
            slot_spec(0),
            slot_spec(1),
            pl.BlockSpec((3, rows, units), lambda i: (0, 0, 0)),
        ],
        out_specs=(
            pl.BlockSpec((wide, units), lambda i: (i, 0)),
            pl.BlockSpec((wide, units), lambda i: (i, 0)),
            pl.BlockSpec((units, wide), lambda i: (0, i)),
        ),
        compiler_params=pltpu.CompilerParams(vmem_limit_bytes=60 * 1000 * 1000),
        name="grads",
    )(slots, slots, hid)
    return output, input_grad, grad_gate[None], grad_up[None], grad_down[None]


def slot_tables(routes, router_weight, experts, capacity):
    expert_ids = jnp.arange(experts, dtype=jnp.int32)
    hit_table = (routes[:, :, None] == expert_ids).astype(jnp.int32)
    per_token = jnp.sum(hit_table, axis=1)
    before = jnp.cumsum(per_token, axis=0) - per_token
    slot_of = jnp.sum(hit_table * before[:, None, :], axis=2)
    slot_ids = jnp.arange(capacity, dtype=jnp.int32)
    placed = hit_table[:, :, :, None] * (slot_of[:, :, None, None] == slot_ids).astype(jnp.int32)
    tok_rows = routes.shape[0]
    flat = placed.reshape(tok_rows, 2, experts * capacity).astype(jnp.float32)
    slot_weight = jnp.sum(flat * router_weight[:, :, None], axis=(0, 1))
    return (flat[:, 0], flat[:, 1], slot_weight)


def on_device(tokens, cotangent, routes, router_weight, w_gate, w_up, w_down):
    experts = lax.axis_size("dp")
    tok_rows, features = tokens.shape
    capacity = max(tok_rows * 3 // 8, tok_rows * 2 // experts, 2)
    local_rows = experts * capacity
    lead = (((0,), (0,)), ((), ()))
    trail = (((1,), (1,)), ((), ()))
    first_pick, second_pick, slot_weight = slot_tables(routes, router_weight, experts, capacity)
    picked = (first_pick + second_pick).astype(jnp.bfloat16)
    send_x = lax.dot_general(picked, tokens, lead, preferred_element_type=jnp.float32).astype(
        jnp.bfloat16
    )
    chosen_dy = lax.dot_general(picked, cotangent, lead, preferred_element_type=jnp.float32)
    send_dy = (chosen_dy * slot_weight[:, None]).astype(jnp.bfloat16)
    arrived_x, arrived_dy = (
        lax.all_to_all(
            send_x.reshape(experts, capacity, features),
            "dp",
            split_axis=0,
            concat_axis=0,
            tiled=True,
        ),
        lax.all_to_all(
            send_dy.reshape(experts, capacity, features),
            "dp",
            split_axis=0,
            concat_axis=0,
            tiled=True,
        ),
    )
    slot_x = arrived_x.reshape(local_rows, features)
    slot_dy = arrived_dy.reshape(local_rows, features)
    gate_w = w_gate[0]
    up_w = w_up[0]
    down_w = w_down[0]
    gate_pre = jnp.dot(slot_x, gate_w, preferred_element_type=jnp.float32)
    up_pre = jnp.dot(slot_x, up_w, preferred_element_type=jnp.float32)
    sigma = jax.nn.sigmoid(gate_pre)
    active = gate_pre * sigma
    hidden = (active * up_pre).astype(jnp.bfloat16)
    out_terms = jnp.dot(hidden, down_w, preferred_element_type=jnp.float32)
    hidden_dy = lax.dot_general(slot_dy, down_w, trail, preferred_element_type=jnp.float32)
    gate_dy = (hidden_dy * up_pre * sigma * (1.0 + gate_pre * (1.0 - sigma))).astype(jnp.bfloat16)
    up_dy = (hidden_dy * active).astype(jnp.bfloat16)
    grad_down = lax.dot_general(hidden, slot_dy, lead, preferred_element_type=jnp.float32).astype(
        jnp.bfloat16
    )
    grad_gate = lax.dot_general(slot_x, gate_dy, lead, preferred_element_type=jnp.float32).astype(
        jnp.bfloat16
    )
    grad_up = lax.dot_general(slot_x, up_dy, lead, preferred_element_type=jnp.float32).astype(
        jnp.bfloat16
    )
    back_terms = lax.dot_general(
        gate_dy, gate_w, trail, preferred_element_type=jnp.float32
    ) + lax.dot_general(up_dy, up_w, trail, preferred_element_type=jnp.float32)
    out_part, back_part = (
        lax.psum_scatter(
            out_terms.reshape(experts, capacity, features).astype(jnp.bfloat16),
            "fsdp",
            scatter_dimension=2,
            tiled=True,
        ).astype(jnp.float32),
        lax.psum_scatter(
            back_terms.reshape(experts, capacity, features).astype(jnp.bfloat16),
            "fsdp",
            scatter_dimension=2,
            tiled=True,
        ).astype(jnp.float32),
    )
    returned_out, returned_dx = (
        lax.all_to_all(
            out_part.astype(jnp.bfloat16), "dp", split_axis=0, concat_axis=0, tiled=True
        ),
        lax.all_to_all(
            back_part.astype(jnp.bfloat16), "dp", split_axis=0, concat_axis=0, tiled=True
        ),
    )
    width = out_part.shape[2]
    flat_out = returned_out.reshape(local_rows, width)
    flat_dx = returned_dx.reshape(local_rows, width)
    first_rows = jnp.dot(
        first_pick.astype(jnp.bfloat16), flat_out, preferred_element_type=jnp.float32
    )
    second_rows = jnp.dot(
        second_pick.astype(jnp.bfloat16), flat_out, preferred_element_type=jnp.float32
    )
    output = (router_weight[:, 0:1] * first_rows + router_weight[:, 1:2] * second_rows).astype(
        jnp.bfloat16
    )
    input_grad = jnp.dot(picked, flat_dx, preferred_element_type=jnp.float32).astype(jnp.bfloat16)
    output, input_grad = (
        lax.all_gather(output, "fsdp", axis=1, tiled=True),
        lax.all_gather(input_grad, "fsdp", axis=1, tiled=True),
    )
    return (output, input_grad, grad_gate[None], grad_up[None], grad_down[None])


def capacity_of(toks, experts):
    return max(toks * 3 // 8, toks * 2 // experts, 2)


def fits(mesh, toks, features, units):
    n, m = mesh.shape["dp"], mesh.shape["fsdp"]
    cap = capacity_of(toks, n)
    powers = n & (n - 1) == 0 and m & (m - 1) == 0 and m >= 4
    whole = features % 1024 == 0 and units % 256 == 0 and cap % 16 == 0 and toks % (8 * m) == 0
    rows = n * cap
    held = 6 * features * units + 2 * rows * (13 * features + 7 * units) + 20 * toks * features
    return powers and whole and held < 56 * 1000 * 1000


def solution(mesh):
    def step(tokens, cotangent, routes, router_weight, w_gate, w_up, w_down):
        body = fused if fits(mesh, *tokens.shape, w_gate.shape[2]) else on_device
        return body(tokens, cotangent, routes, router_weight, w_gate, w_up, w_down)

    return jax.shard_map(
        step,
        mesh=mesh,
        in_specs=(
            P("dp", None),
            P("dp", None),
            P("dp", None),
            P("dp", None),
            P("dp", None, "fsdp"),
            P("dp", None, "fsdp"),
            P("dp", "fsdp", None),
        ),
        out_specs=(
            P("dp", None),
            P("dp", None),
            P("dp", None, "fsdp"),
            P("dp", None, "fsdp"),
            P("dp", "fsdp", None),
        ),
        check_vma=False,
    )
```
